32 devices in a mesh: grp: 2 (over y), seq: 4 (over z), head: 4 (over x, core).
Axes of the slice: x: 2, y: 2, z: 4, core: 2. Of those that a mesh axis runs over, the one named last changes fastest.
Arguments:
- queries: bfloat16 [1024, 32, 128], P(('grp', 'seq'), 'head'), parts along dimension 0, may hold values from -26 to 26
- keys: bfloat16 [1024, 8, 128], P(('grp', 'seq'), 'head'), parts along dimension 0, may hold values from -13 to 13
- values: bfloat16 [1024, 8, 128], P(('grp', 'seq'), 'head'), parts along dimension 0, may hold values from -6 to 6
- block_order: int32 [16], P('grp'), parts along dimension 0, may hold values from 0 to 7, as said below
Outputs:
- attended: bfloat16 [1024, 32, 128], P(('grp', 'seq'), 'head'), parts along dimension 0
The draws below stay inside these ranges and needn't reach their ends.
There are 2 independent parts, one for each index of `grp`. The reference program is written for one: setup_inputs(seed, part) draws one part's arguments, and reference() takes and returns one part's arrays. A program takes and returns all parts, laid end to end along the dimension named above; each array names one. Nothing has to cross between parts.
Inputs may be any that keep to these rules, and one draw needn't show every extreme that they name: `block_order`: slots 2 i and 2 i + 1 hold blocks c and 7 - c for some c, in either order; every block stands in one slot.
All inputs are finite; a program needn't handle non-finite values.
Results may differ from the reference program's by a relative error of at most 0.0055.
Values may be sent and summed in bfloat16 or wider, within the bound.
A program may use at most 128 MiB of HBM per device.

```python
import jax
import jax.numpy as jnp
from jax import lax

QH = 32
KVH = 8
HD = 128
TOK_DEV = 128
BLOCK = 64
TOKENS = 512
N_SEQ = 4


def pair_order(key):
    count = N_SEQ
    shuffled = jax.random.permutation(jax.random.fold_in(key, 11), count).astype(jnp.int32)
    flips = jax.random.randint(jax.random.fold_in(key, 12), (count,), 0, 2).astype(jnp.int32)
    first = jnp.where(flips == 0, shuffled, 2 * count - 1 - shuffled)
    second = 2 * count - 1 - first
    return jnp.stack([first, second], axis=1).reshape(2 * count).astype(jnp.int32)


def draw_block_order(key, part):
    return pair_order(key)


def draw_queries(key, part):
    base = jnp.clip(jax.random.normal(jax.random.fold_in(key, 21), (TOKENS, QH, HD), jnp.float32), -5.0, 5.0)
    return base.astype(jnp.bfloat16)


def draw_keys(key, part):
    base = jnp.clip(jax.random.normal(jax.random.fold_in(key, 22), (TOKENS, KVH, HD), jnp.float32), -5.0, 5.0)
    return base.astype(jnp.bfloat16)


def levels(stream_key, shape, cuts, smallest, largest):
    gain = 1.0
    for position, parts in cuts:
        steps = jax.random.uniform(jax.random.fold_in(jax.random.fold_in(stream_key, 6), position), (parts,), jnp.float32, smallest / len(cuts), largest / len(cuts))
        gain = gain * jnp.repeat(jnp.exp(steps), shape[position] // parts).reshape((-1,) + (1,) * (len(shape) - 1 - position))
    return gain


def normal_values(own_key, shape, spread, most, pieces=(), kind=jnp.bfloat16):
    factor_of = levels(own_key, shape, pieces, -0.22, 0.18) if pieces else 1.0
    values = jax.random.normal(own_key, shape, jnp.float32) * spread * factor_of
    return jnp.minimum(jnp.maximum(values, -most), most).astype(kind)


def setup_inputs(seed: int = 0, part: int = 0) -> dict:
    arg_keys = jax.random.split(jax.random.key(seed), 5)
    part_splits = jax.random.split(jax.random.fold_in(arg_keys[4], part), 5)
    return {
        "queries": draw_queries(jax.random.fold_in(jax.random.fold_in(arg_keys[4], part), 71), part),
        "keys": draw_keys(jax.random.fold_in(jax.random.fold_in(arg_keys[4], part), 71), part),
        "values": normal_values(part_splits[2], (TOKENS, KVH, HD), 1.0, 6.0, ((0, 4), (1, 4))),
        "block_order": draw_block_order(jax.random.fold_in(jax.random.fold_in(arg_keys[4], part), 71), part),
    }


def reference(queries, keys, values, block_order):
    rows = jnp.arange(TOKENS, dtype=jnp.int32)
    positions = block_order[rows // BLOCK].astype(jnp.int32) * BLOCK + rows % BLOCK
    key_float = keys.astype(jnp.float32)
    value_float = values.astype(jnp.float32)
    group_size = QH // KVH
    score_scale = HD ** -0.5

    def one_block(index):
        start = (index * TOK_DEV).astype(jnp.int32)
        query_rows = lax.dynamic_slice_in_dim(queries, start, TOK_DEV, 0).astype(jnp.float32)
        query_rows = query_rows.reshape(TOK_DEV, KVH, group_size, HD)
        query_pos = lax.dynamic_slice_in_dim(positions, start, TOK_DEV, 0)
        scores = jnp.einsum("cghd,pgd->ghcp", query_rows, key_float) * score_scale
        visible = (positions[None, :] <= query_pos[:, None])[None, None]
        top = jnp.max(jnp.where(visible, scores, -1e30), axis=-1)
        weights = jnp.where(visible, jnp.exp(scores - top[..., None]), 0.0)
        total = jnp.sum(weights, axis=-1)
        rounded = lax.optimization_barrier(weights.astype(jnp.bfloat16)).astype(jnp.float32)
        summed = jnp.einsum("ghcp,pgd->ghcd", rounded, value_float)
        result = summed / total[..., None]
        return jnp.transpose(result, (2, 0, 1, 3)).reshape(TOK_DEV, QH, HD).astype(jnp.bfloat16)

    blocks = lax.map(one_block, jnp.arange(N_SEQ, dtype=jnp.int32))
    return blocks.reshape(TOKENS, QH, HD)
```

```python
import functools
import math

import jax
import jax.numpy as jnp
from jax import lax
from jax.experimental import pallas as pl
from jax.experimental.pallas import tpu as pltpu
from jax.sharding import PartitionSpec as P

MESH = pl.DeviceIdType.MESH
NEG = -1e30

PLANS = (
    (((), ()),),
    ((((1, ((1, 0),), ((1, 1),)),), ((1, ((1, 0),), ((1, 1),)),)), (((0, ((0, 0),), ((0, 1),)),), ((0, ((0, 0),), ((0, 1),)),))),
    ((((1, ((1, 0), (1, 1)), ()), (2, ((2, 0),), ((2, 1),))), ((1, ((1, 0), (1, 1)), ()), (2, ((2, 0),), ((2, 1),)))), (((0, ((0, 0), (0, 1)), ()), (2, ((2, 0),), ((2, 1),))), ((0, ((0, 0), (0, 1)), ()), (2, ((2, 0),), ((2, 1),)))), (((1, ((1, 0), (1, 1)), ()), (0, ((0, 0),), ((0, 1),))), ((1, ((1, 0), (1, 1)), ()), (0, ((0, 0),), ((0, 1),))))),
    ((((1, ((1, 0), (1, 1)), ()), (2, ((2, 0), (2, 1)), ()), (3, ((3, 0),), ((3, 1),))), ((1, ((1, 0), (1, 1)), ()), (2, ((2, 0), (2, 1)), ()), (3, ((3, 0),), ((3, 1),)))), (((3, ((3, 0), (3, 1)), ()), (0, ((0, 0), (0, 1)), ()), (2, ((2, 0),), ((2, 1),))), ((3, ((3, 0), (3, 1)), ()), (0, ((0, 0), (0, 1)), ()), (2, ((2, 0),), ((2, 1),)))), (((0, ((0, 0), (0, 1)), ()), (3, ((3, 0), (3, 1)), ()), (1, ((1, 0),), ((1, 1),))), ((0, ((0, 0), (0, 1)), ()), (3, ((3, 0), (3, 1)), ()), (1, ((1, 0),), ((1, 1),)))), (((2, ((2, 0), (2, 1)), ()), (1, ((1, 0), (1, 1)), ()), (0, ((0, 0),), ((0, 1),))), ((2, ((2, 0), (2, 1)), ()), (1, ((1, 0), (1, 1)), ()), (0, ((0, 0),), ((0, 1),))))),
)


def gather_attend(
    n,
    heads,
    groups,
    tile,
    table_hbm,
    q_hbm,
    k_hbm,
    v_hbm,
    out_ref,
    table_ref,
    q_ref,
    kv_ref,
    p_ref,
    m_ref,
    l_ref,
    acc_ref,
    wide_ref,
    keys_ref,
    values_ref,
    load_sem,
    send_sem,
    recv_sem,
    ready_sem,
):
    me = lax.axis_index("seq")
    rows, width = q_ref.shape
    tokens = rows // heads
    half = tokens // 2
    per_group = heads // groups
    cols = tokens * groups
    pieces = recv_sem.shape[1]
    piece = 2 * cols // pieces
    factor_scale = width ** (-0.5) * math.log2(math.e)
    has_right, has_left = me < n - 1, me > 0
    barrier = pltpu.get_barrier_semaphore()
    odd = lax.axis_index("head") % 2 == 1
    reach = min(2, n - 1)

    loads = [
        pltpu.make_async_copy(k_hbm, kv_ref.at[me, 0], load_sem.at[0]),
        pltpu.make_async_copy(v_hbm, kv_ref.at[me, 1], load_sem.at[0]),
        pltpu.make_async_copy(table_hbm, table_ref, load_sem.at[1]),
        pltpu.make_async_copy(q_hbm, q_ref, load_sem.at[2]),
    ]
    for load in loads:
        load.start()

    def present(device):
        return (device >= 0) & (device < n)

    for k in range(1, reach + 1):

        @pl.when(present(me + k))
        def _():
            pl.semaphore_signal(barrier, inc=1, device_id={"seq": me + k}, device_id_type=MESH)

    @pl.when(has_left)
    def _():
        pl.semaphore_wait(barrier, jnp.minimum(me, reach))

    for k in range(1, reach + 1):

        @pl.when(present(me - k))
        def _():
            pl.semaphore_signal(
                ready_sem.at[k - 1], inc=1, device_id={"seq": me - k}, device_id_type=MESH
            )

    def part(shard, which):
        per = pieces // 2
        return kv_ref.at[shard, which // per, pl.ds((which % per) * piece, piece)]

    def remote(shard, which, target):
        slot = jnp.where(shard < target, shard, shard - 1)
        return pltpu.make_async_remote_copy(
            src_ref=part(shard, which),
            dst_ref=part(shard, which),
            send_sem=send_sem.at[jnp.where(target < me, 0, 1)],
            recv_sem=recv_sem.at[slot, which],
            device_id={"seq": target},
            device_id_type=MESH,
        )

    pltpu.make_async_copy(kv_ref.at[me], kv_ref.at[me], load_sem.at[0]).wait()

    for k in range(reach, 0, -1):

        @pl.when(present(me - k))
        def _():
            for which in range(pieces):
                remote(me, which, me - k).start()

    m_ref[...] = jnp.full(m_ref.shape, NEG, jnp.float32)
    l_ref[...] = jnp.zeros(l_ref.shape, jnp.float32)
    acc_ref[...] = jnp.zeros(acc_ref.shape, jnp.float32)
    loads[2].wait()
    loads[3].wait()

    lane = lax.broadcasted_iota(jnp.int32, (heads, tokens), 1)
    group = lax.broadcasted_iota(jnp.int32, (heads, tokens), 0) // per_group

    def by_group(shard, side):
        wide_ref[...] = kv_ref[shard, side].astype(jnp.float32)
        split = [wide_ref[pl.ds(g, tokens, stride=groups), :] for g in range(groups)]
        return jnp.concatenate(split, axis=0).astype(kv_ref.dtype)

    def scores(shard, keys, section, start):
        span = pl.ds((section * half + start) * heads, tile * heads)
        first, second = table_ref[2 * shard], table_ref[2 * shard + 1]
        key_pos = jnp.where(lane < half, first * half + lane, (second - 1) * half + lane)
        offset = table_ref[2 * me + section] * half + start
        raw = lax.dot_general(
            q_ref[span, :],
            keys,
            (((1,), (1,)), ((), ())),
            preferred_element_type=jnp.float32,
        )
        raw = raw.reshape(tile, heads, cols)
        shaped = raw[:, :, :tokens]
        for g in range(1, groups):
            shaped = jnp.where(group[None] == g, raw[:, :, g * tokens : (g + 1) * tokens], shaped)
        query_pos = lax.broadcasted_iota(jnp.int32, shaped.shape, 0) + offset
        shaped = jnp.where(key_pos[None] <= query_pos, shaped, NEG)
        raw = shaped.reshape(tile * heads, tokens)
        old_max = m_ref[span, :]
        new_max = jnp.maximum(old_max, jnp.max(raw, axis=-1, keepdims=True))
        fade = jnp.exp2((old_max - new_max) * factor_scale)
        weights = jnp.exp2((raw - new_max) * factor_scale)
        m_ref[span, :] = new_max
        l_ref[span, :] = l_ref[span, :] * fade + weights
        shaped = weights.reshape(tile, heads, tokens)
        spread = [jnp.where(group[None] == g, shaped, 0.0) for g in range(groups)]
        spread = jnp.concatenate(spread, axis=-1).reshape(tile * heads, cols)
        return span, spread.astype(p_ref.dtype), fade

    def whole(shard):
        keys_ref[...] = by_group(shard, 0)
        values_ref[...] = by_group(shard, 1)

        for start in range(0, tokens, tile):
            span, weights, fade = scores(shard, keys_ref[...], start // half, start % half)
            acc_ref[span, :] = acc_ref[span, :] * fade + jnp.dot(
                weights, values_ref[...], preferred_element_type=jnp.float32
            )

    whole(me)

    for k in range(1, reach + 1):

        @pl.when(present(me + k))
        def _():
            with jax.named_scope(f"ready{k}"):
                pl.semaphore_wait(ready_sem.at[k - 1], 1)
            for which in range(pieces):
                remote(me, which, me + k).start()

    def passes_right(shard):
        return has_right & (me - shard >= reach)

    def passes_left(shard):
        return has_left & (shard - me >= reach)

    def take(shard, which):
        with jax.named_scope(f"take{which}"):
            remote(shard, which, me).wait_recv()

        @pl.when(passes_right(shard))
        def _():
            remote(shard, which, me + 1).start()

        @pl.when(passes_left(shard))
        def _():
            remote(shard, which, me - 1).start()

    def settle():
        for d in range(n):
            to_left = min(d, reach) + (max(n - 1 - d - (reach - 1), 0) if d > 0 else 0)
            to_right = min(n - 1 - d, reach) + (max(d - (reach - 1), 0) if d < n - 1 else 0)

            @pl.when(me == d)
            def _():
                for side, count in enumerate((to_left, to_right)):
                    if count:
                        sent = kv_ref.at[pl.ds(0, count)]
                        pltpu.make_async_copy(sent, sent, send_sem.at[side]).wait()

    if n == 1:
        for start in range(0, tokens, tile):
            span = pl.ds(start * heads, tile * heads)
            scale = 1.0 / jnp.sum(l_ref[span, :], axis=-1, keepdims=True)
            out_ref[span, :] = (acc_ref[span, :] * scale).astype(out_ref.dtype)
        return

    early, late = range(pieces // 2), range(pieces // 2, pieces)

    if n <= len(PLANS):
        variants = [
            ((me == d) & (odd == (parity == 1)), PLANS[n - 1][d][parity])
            for d in range(n)
            for parity in range(2)
        ]

        def shard_at(index):
            return sum(jnp.where(mine, plan[index][0], 0) for mine, plan in variants)

        def takes_at(index, side):
            for mine, plan in variants:
                taken = [t for t in plan[index][1 + side]]
                if taken:

                    @pl.when(mine)
                    def _():
                        for shard, half_of in taken:
                            for which in (early, late)[half_of]:
                                take(shard, which)

        for index in range(n - 2):
            takes_at(index, 0)
            whole(shard_at(index))
        takes_at(n - 2, 0)
        last = shard_at(n - 2)
    else:
        short = jnp.minimum(me, n - 1 - me)
        middle = has_left & has_right

        def order(index):
            paired = jnp.where(index % 2 == 1, me + (index + 1) // 2, me - index // 2)
            alone = jnp.where(me < n - 1 - me, me + index - short, me - index + short)
            return jnp.where(index <= 2 * short, paired, alone)

        def take_all(index):
            for which in range(pieces):
                take(order(index), which)

        def round_of(index, carry):
            @pl.when(middle)
            def _():
                take_all(index + 1)

            whole(order(index))

            @pl.when(jnp.logical_not(middle))
            def _():
                take_all(index + 1)

            return carry

        take_all(1)
        lax.fori_loop(1, n - 2, round_of, 0)
        whole(order(n - 2))
        last = order(n - 1)
        for which in early:
            take(last, which)

        def takes_at(index, side):
            for which in late:
                take(last, which)

    keys_ref[...] = by_group(last, 0)
    for start in range(0, tokens, tile):
        span, weights, fade = scores(last, keys_ref[...], start // half, start % half)
        scale = 1.0 / jnp.sum(l_ref[span, :], axis=-1, keepdims=True)
        p_ref[span, :] = weights
        acc_ref[span, :] = acc_ref[span, :] * (fade * scale)
        l_ref[span, :] = jnp.broadcast_to(scale, (tile * heads, width))

    takes_at(n - 2, 1)
    values_ref[...] = by_group(last, 1)
    for start in range(0, tokens, tile):
        span = pl.ds(start * heads, tile * heads)
        product = jnp.dot(p_ref[span, :], values_ref[...], preferred_element_type=jnp.float32)
        out_ref[span, :] = (acc_ref[span, :] + product * l_ref[span, :]).astype(out_ref.dtype)
    settle()


def on_device(queries, keys, values, block_order):
    n = lax.axis_size("seq")
    tokens, heads, width = queries.shape
    groups = keys.shape[1]
    rows, cols = tokens * heads, tokens * groups
    tile = min(64, tokens // 2)
    pieces = 4
    anywhere = pl.BlockSpec(memory_space=pltpu.HBM)
    out = pl.pallas_call(
        functools.partial(gather_attend, n, heads, groups, tile),
        out_shape=pltpu.VMEM((rows, width), queries.dtype),
        in_specs=[anywhere] * 4,
        out_specs=pl.BlockSpec(memory_space=pltpu.VMEM),
        scratch_shapes=[
            pltpu.SMEM(block_order.shape, block_order.dtype),
            pltpu.VMEM((rows, width), queries.dtype),
            pltpu.VMEM((n, 2, cols, width), keys.dtype),
            pltpu.VMEM((rows, cols), values.dtype),
            pltpu.VMEM((rows, width), jnp.float32),
            pltpu.VMEM((rows, width), jnp.float32),
            pltpu.VMEM((rows, width), jnp.float32),
            pltpu.VMEM((cols, width), jnp.float32),
            pltpu.VMEM((cols, width), keys.dtype),
            pltpu.VMEM((cols, width), values.dtype),
            pltpu.SemaphoreType.DMA((3,)),
            pltpu.SemaphoreType.DMA((2,)),
            pltpu.SemaphoreType.DMA((max(n - 1, 1), pieces)),
            pltpu.SemaphoreType.REGULAR((2,)),
        ],
        compiler_params=pltpu.CompilerParams(collective_id=0, has_side_effects=True),
    )(
        block_order,
        queries.reshape(rows, width),
        keys.reshape(cols, width),
        values.reshape(cols, width),
    )
    return out.reshape(tokens, heads, width)


def solution(mesh):
    placed = P(("grp", "seq"), "head", None)
    return jax.shard_map(
        on_device,
        mesh=mesh,
        in_specs=(placed, placed, placed, P("grp")),
        out_specs=placed,
        check_vma=False,
    )
```

```python
import functools
import math

import jax
import jax.numpy as jnp
from jax import lax
from jax.experimental import pallas as pl
from jax.experimental.pallas import tpu as pltpu
from jax.sharding import PartitionSpec as P

MESH = pl.DeviceIdType.MESH
NEG = -1e30
KEYS, VALUES = 0, 1

LINE_OF_FOUR = (
    (
        (1, 3, 2, 0, (((1, KEYS), (1, VALUES)), ((3, KEYS),), ((3, VALUES),), ((2, KEYS),), ((2, VALUES),))),
        (1, 3, 2, 1, (((1, KEYS), (1, VALUES)), ((2, KEYS),), ((3, KEYS),), ((3, VALUES),), ((2, VALUES),))),
    ),
    (
        (0, 3, 2, 1, (((0, KEYS), (0, VALUES)), ((2, KEYS),), ((3, KEYS),), ((3, VALUES),), ((2, VALUES),))),
        (3, 2, 0, 0, (((2, KEYS), (3, KEYS), (3, VALUES), (2, VALUES)), (), (), ((0, KEYS),), ((0, VALUES),))),
    ),
    (
        (0, 3, 1, 0, (((0, KEYS), (0, VALUES)), ((3, KEYS),), ((3, VALUES),), ((1, KEYS),), ((1, VALUES),))),
        (0, 3, 1, 0, (((0, KEYS), (0, VALUES)), ((3, KEYS),), ((3, VALUES),), ((1, KEYS),), ((1, VALUES),))),
    ),
    (
        (2, 1, 0, 0, (((2, KEYS), (2, VALUES)), ((1, KEYS),), ((1, VALUES),), ((0, KEYS),), ((0, VALUES),))),
        (2, 1, 0, 0, (((2, KEYS), (2, VALUES)), ((1, KEYS),), ((1, VALUES),), ((0, KEYS),), ((0, VALUES),))),
    ),
)


def gather_attend(
    n,
    heads,
    groups,
    tile,
    table_hbm,
    q_hbm,
    k_hbm,
    v_hbm,
    out_ref,
    table_ref,
    q_ref,
    kv_ref,
    p_ref,
    m_ref,
    l_ref,
    acc_ref,
    scale_ref,
    wide_ref,
    keys_ref,
    values_ref,
    load_sem,
    send_sem,
    recv_sem,
    ready_sem,
):
    me = lax.axis_index("seq")
    odd = lax.axis_index("head") % 2 == 1
    rows, width = q_ref.shape
    tokens = rows // heads
    half = tokens // 2
    per_group = heads // groups
    cols = tokens * groups
    per_side = recv_sem.shape[1] // 2
    piece = cols // per_side
    factor_scale = width ** (-0.5) * math.log2(math.e)
    has_right, has_left = me < n - 1, me > 0
    reach_left, reach_right = min(3, n - 1), min(2, n - 1)
    barrier = pltpu.get_barrier_semaphore()

    loads = [
        pltpu.make_async_copy(k_hbm, kv_ref.at[me, KEYS], load_sem.at[0]),
        pltpu.make_async_copy(v_hbm, kv_ref.at[me, VALUES], load_sem.at[0]),
        pltpu.make_async_copy(table_hbm, table_ref, load_sem.at[1]),
        pltpu.make_async_copy(q_hbm, q_ref, load_sem.at[2]),
    ]
    for load in loads:
        load.start()

    def straight_left(high, low, is_odd):
        far = high - low
        even_way = far <= reach_left
        odd_way = (far == 1) | ((far == 2) & (high == n - 1))
        return (low >= 0) & (high < n) & ((is_odd & odd_way) | (jnp.logical_not(is_odd) & even_way))

    def straight_right(low, high):
        return (low >= 0) & (high < n) & (high - low <= reach_right)

    def meets(high, low):
        return straight_left(high, low, odd) | straight_right(low, high)

    for k in range(1, reach_left + 1):

        @pl.when(meets(me + k, me))
        def _():
            pl.semaphore_signal(barrier, inc=1, device_id={"seq": me + k}, device_id_type=MESH)

    greeted = [meets(me, me - k).astype(jnp.int32) for k in range(1, reach_left + 1)]

    @pl.when(has_left)
    def _():
        pl.semaphore_wait(barrier, sum(greeted))

    for k in range(1, reach_right + 1):

        @pl.when(straight_right(me - k, me))
        def _():
            pl.semaphore_signal(
                ready_sem.at[k - 1], inc=1, device_id={"seq": me - k}, device_id_type=MESH
            )

    def remote(shard, side, index, target, source=None):
        part = kv_ref.at[shard, side, pl.ds(index * piece, piece)]
        slot = jnp.where(shard < target, shard, shard - 1)
        return pltpu.make_async_remote_copy(
            src_ref=part if source is None else source.at[pl.ds(index * piece, piece)],
            dst_ref=part,
            send_sem=send_sem.at[jnp.where(target < me, 0, 1)],
            recv_sem=recv_sem.at[slot, side * per_side + index],
            device_id={"seq": target},
            device_id_type=MESH,
        )

    def send_mine(target, allowed, sources=(None, None)):
        @pl.when(allowed)
        def _():
            for side in (KEYS, VALUES):
                for index in range(per_side):
                    remote(me, side, index, target, sources[side]).start()

    for k, rank in ((3, None), (2, False), (1, None), (2, True)):
        if k <= reach_left:
            turn = straight_left(me, me - k, odd)
            if rank is not None:
                turn &= (jnp.logical_not(odd) & (me == n - 1)) == rank
            send_mine(me - k, turn, (k_hbm, v_hbm))

    m_ref[...] = jnp.full(m_ref.shape, NEG, jnp.float32)
    l_ref[...] = jnp.zeros(l_ref.shape, jnp.float32)
    acc_ref[...] = jnp.zeros(acc_ref.shape, jnp.float32)
    pltpu.make_async_copy(kv_ref.at[me], kv_ref.at[me], load_sem.at[0]).wait()
    loads[2].wait()
    loads[3].wait()

    lane = lax.broadcasted_iota(jnp.int32, (heads, tokens), 1)
    group = lax.broadcasted_iota(jnp.int32, (heads, tokens), 0) // per_group
    spans = [(pl.ds(start * heads, tile * heads), start) for start in range(0, tokens, tile)]

    def by_group(shard, side):
        wide_ref[...] = kv_ref[shard, side].astype(jnp.float32)
        split = [wide_ref[pl.ds(g, tokens, stride=groups), :] for g in range(groups)]
        return jnp.concatenate(split, axis=0).astype(kv_ref.dtype)

    def scores(shard, span, start):
        section = start // half
        first, second = table_ref[2 * shard], table_ref[2 * shard + 1]
        key_pos = jnp.where(lane < half, first * half + lane, (second - 1) * half + lane)
        offset = table_ref[2 * me + section] * half + start % half
        raw = lax.dot_general(
            q_ref[span, :],
            keys_ref[...],
            (((1,), (1,)), ((), ())),
            preferred_element_type=jnp.float32,
        )
        raw = raw.reshape(tile, heads, cols)
        shaped = raw[:, :, :tokens]
        for g in range(1, groups):
            shaped = jnp.where(group[None] == g, raw[:, :, g * tokens : (g + 1) * tokens], shaped)
        query_pos = lax.broadcasted_iota(jnp.int32, shaped.shape, 0) + offset
        shaped = jnp.where(key_pos[None] <= query_pos, shaped, NEG)
        raw = shaped.reshape(tile * heads, tokens)
        old_max = m_ref[span, :]
        new_max = jnp.maximum(old_max, jnp.max(raw, axis=-1, keepdims=True))
        fade = jnp.exp2((old_max - new_max) * factor_scale)
        weights = jnp.exp2((raw - new_max) * factor_scale)
        m_ref[span, :] = new_max
        l_ref[span, :] = l_ref[span, :] * fade + weights
        shaped = weights.reshape(tile, heads, tokens)
        spread = [jnp.where(group[None] == g, shaped, 0.0) for g in range(groups)]
        spread = jnp.concatenate(spread, axis=-1).reshape(tile * heads, cols)
        return spread.astype(p_ref.dtype), fade

    def scale_of(span):
        high = l_ref[span, :].astype(p_ref.dtype)
        low = (l_ref[span, :] - high.astype(jnp.float32)).astype(p_ref.dtype)
        ones = jnp.ones((2 * tokens, width), p_ref.dtype)
        return 1.0 / jnp.dot(
            jnp.concatenate([high, low], axis=1), ones, preferred_element_type=jnp.float32
        )

    def whole(shard):
        keys_ref[...] = by_group(shard, KEYS)
        values_ref[...] = by_group(shard, VALUES)
        for span, start in spans:
            weights, fade = scores(shard, span, start)
            acc_ref[span, :] = acc_ref[span, :] * fade + jnp.dot(
                weights, values_ref[...], preferred_element_type=jnp.float32
            )

    def weigh(shard, place, closes):
        keys_ref[...] = by_group(shard, KEYS)
        for span, start in spans:
            weights, fade = scores(shard, span, start)
            p_ref[place, span, :] = weights
            if closes:
                scale = scale_of(span)
                scale_ref[1, span, :] = scale
                fade *= scale
                scale_ref[0, span, :] = fade
            acc_ref[span, :] = acc_ref[span, :] * fade

    def product(span, place):
        return jnp.dot(p_ref[place, span, :], values_ref[...], preferred_element_type=jnp.float32)

    def add(shard, place, scales):
        values_ref[...] = by_group(shard, VALUES)
        for span, _ in spans:
            term = product(span, place)
            if scales:
                term *= scale_ref[1, span, :]
            acc_ref[span, :] += term

    whole(me)

    far_first = (me == n - 3) & jnp.logical_not(odd)
    for k, rank in ((1, False), (2, None), (1, True)):
        if k <= reach_right:
            turn = straight_right(me, me + k)
            if rank is not None:
                turn &= far_first == rank

            @pl.when(turn)
            def _():
                pl.semaphore_wait(ready_sem.at[k - 1], 1)

            send_mine(me + k, turn)

    def take(shard, side):
        for index in range(per_side):
            remote(shard, side, index, me).wait_recv()

            @pl.when(has_right & (shard < me) & jnp.logical_not(straight_right(shard, me + 1)))
            def _():
                remote(shard, side, index, me + 1).start()

            @pl.when(has_left & (shard > me) & jnp.logical_not(straight_left(shard, me - 1, odd)))
            def _():
                remote(shard, side, index, me - 1).start()

    def settle():
        for d in range(n):
            for is_odd in (False, True):
                lefts = [s for s in range(d + 1, n) if d > 0]
                if is_odd:
                    lefts = [s for s in lefts if not (s == n - 1 and s - d == 1)]
                    own_left = min(d, 2 if d == n - 1 else 1)
                else:
                    lefts = [s for s in lefts if s - d + 1 > reach_left]
                    own_left = min(d, reach_left)
                rights = [s for s in range(d) if d < n - 1 and d + 1 - s > reach_right]
                own_right = min(n - 1 - d, reach_right)
                counts = (own_left + len(lefts), own_right + len(rights))

                @pl.when((me == d) & (odd == is_odd))
                def _():
                    for way, count in enumerate(counts):
                        if count:
                            sent = kv_ref.at[pl.ds(0, count)]
                            pltpu.make_async_copy(sent, sent, send_sem.at[way]).wait()

    if n == 1:
        for span, _ in spans:
            out_ref[span, :] = (acc_ref[span, :] * scale_of(span)).astype(out_ref.dtype)
        return

    def attend_in_turn(second, last, wait_for):
        if second is not None:
            wait_for(1)
            weigh(second, 1, False)
            wait_for(2)
            add(second, 1, False)
        wait_for(3)
        weigh(last, 0, True)

    if n == len(LINE_OF_FOUR):
        variants = [
            ((me == d) & (odd == (parity == 1)), LINE_OF_FOUR[d][parity])
            for d in range(n)
            for parity in range(2)
        ]
        first, second, last, split = (
            sum(jnp.where(mine, plan[field], 0) for mine, plan in variants) for field in range(4)
        )

        def wait_for(stage, kinds=(0, 1)):
            for mine, plan in variants:
                if plan[3] in kinds and plan[4][stage]:

                    @pl.when(mine)
                    def _():
                        for shard, side in plan[4][stage]:
                            take(shard, side)

        wait_for(0)
        whole(first)

        @pl.when(split == 0)
        def _():
            attend_in_turn(second, last, functools.partial(wait_for, kinds=(0,)))

        @pl.when(split == 1)
        def _():
            wait_for(1, (1,))
            weigh(last, 0, False)
            wait_for(2, (1,))
            weigh(second, 1, True)
            wait_for(3, (1,))
            add(second, 1, True)

        wait_for(4)
        factor = jnp.where(split == 1, 0, 1)
    else:
        short = jnp.minimum(me, n - 1 - me)

        def order(index):
            paired = jnp.where(index % 2 == 1, me + (index + 1) // 2, me - index // 2)
            alone = jnp.where(me < n - 1 - me, me + index - short, me - index + short)
            return jnp.where(index <= 2 * short, paired, alone)

        def take_both(index):
            take(order(index), KEYS)
            take(order(index), VALUES)

        def round_of(index, carry):
            take_both(index + 1)
            whole(order(index))
            return carry

        if n > 3:
            take_both(1)
            lax.fori_loop(1, n - 3, round_of, 0)
            whole(order(n - 3))
        last = order(n - 1)

        def wait_for(stage):
            take(order(n - 2) if stage < 3 else last, (stage + 1) % 2)

        attend_in_turn(order(n - 2) if n > 2 else None, last, wait_for)
        wait_for(4)
        factor = 1

    values_ref[...] = by_group(last, VALUES)
    for span, _ in spans:
        out_ref[span, :] = (acc_ref[span, :] + product(span, 0) * scale_ref[factor, span, :]).astype(
            out_ref.dtype
        )
    settle()


def on_device(queries, keys, values, block_order):
    n = lax.axis_size("seq")
    tokens, heads, width = queries.shape
    groups = keys.shape[1]
    rows, cols = tokens * heads, tokens * groups
    tile = min(64, tokens // 2)
    pieces = 4
    anywhere = pl.BlockSpec(memory_space=pltpu.HBM)
    out = pl.pallas_call(
        functools.partial(gather_attend, n, heads, groups, tile),
        out_shape=pltpu.VMEM((rows, width), queries.dtype),
        in_specs=[anywhere] * 4,
        out_specs=pl.BlockSpec(memory_space=pltpu.VMEM),
        scratch_shapes=[
            pltpu.SMEM(block_order.shape, block_order.dtype),
            pltpu.VMEM((rows, width), queries.dtype),
            pltpu.VMEM((n, 2, cols, width), keys.dtype),
            pltpu.VMEM((2, rows, cols), values.dtype),
            pltpu.VMEM((rows, width), jnp.float32),
            pltpu.VMEM((rows, width), jnp.float32),
            pltpu.VMEM((rows, width), jnp.float32),
            pltpu.VMEM((2, rows, width), jnp.float32),
            pltpu.VMEM((cols, width), jnp.float32),
            pltpu.VMEM((cols, width), keys.dtype),
            pltpu.VMEM((cols, width), values.dtype),
            pltpu.SemaphoreType.DMA((3,)),
            pltpu.SemaphoreType.DMA((2,)),
            pltpu.SemaphoreType.DMA((max(n - 1, 1), pieces)),
            pltpu.SemaphoreType.REGULAR((2,)),
        ],
        compiler_params=pltpu.CompilerParams(collective_id=0, has_side_effects=True),
    )(
        block_order,
        queries.reshape(rows, width),
        keys.reshape(cols, width),
        values.reshape(cols, width),
    )
    return out.reshape(tokens, heads, width)


def solution(mesh):
    placed = P(("grp", "seq"), "head", None)
    return jax.shard_map(
        on_device,
        mesh=mesh,
        in_specs=(placed, placed, placed, P("grp")),
        out_specs=placed,
        check_vma=False,
    )
```

```python
import functools
import math

import jax
import jax.numpy as jnp
from jax import lax
from jax.experimental import pallas as pl
from jax.experimental.pallas import tpu as pltpu
from jax.sharding import PartitionSpec as P

MESH = pl.DeviceIdType.MESH
NEG = -1e30
KEYS, VALUES = 0, 1

LINE_OF_FOUR = (
    (
        (1, 3, 2, 0, (((1, KEYS), (1, VALUES)), ((3, KEYS),), ((3, VALUES),), ((2, KEYS),), ((2, VALUES),))),
        (1, 3, 2, 1, (((1, KEYS), (1, VALUES)), ((2, KEYS),), ((3, KEYS),), ((3, VALUES),), ((2, VALUES),))),
    ),
    (
        (0, 3, 2, 1, (((0, KEYS), (0, VALUES)), ((2, KEYS),), ((3, KEYS),), ((3, VALUES),), ((2, VALUES),))),
        (3, 2, 0, 0, (((2, KEYS), (3, KEYS), (3, VALUES), (2, VALUES)), (), (), ((0, KEYS),), ((0, VALUES),))),
    ),
    (
        (0, 3, 1, 0, (((0, KEYS), (0, VALUES)), ((3, KEYS),), ((3, VALUES),), ((1, KEYS),), ((1, VALUES),))),
        (0, 3, 1, 0, (((0, KEYS), (0, VALUES)), ((3, KEYS),), ((3, VALUES),), ((1, KEYS),), ((1, VALUES),))),
    ),
    (
        (2, 1, 0, 0, (((2, KEYS), (2, VALUES)), ((1, KEYS),), ((1, VALUES),), ((0, KEYS),), ((0, VALUES),))),
        (2, 1, 0, 0, (((2, KEYS), (2, VALUES)), ((1, KEYS),), ((1, VALUES),), ((0, KEYS),), ((0, VALUES),))),
    ),
)


def gather_attend(
    n,
    heads,
    groups,
    tile,
    table_hbm,
    q_hbm,
    k_hbm,
    v_hbm,
    out_ref,
    table_ref,
    q_ref,
    kv_ref,
    p_ref,
    m_ref,
    l_ref,
    acc_ref,
    scale_ref,
    wide_ref,
    keys_ref,
    values_ref,
    load_sem,
    send_sem,
    recv_sem,
    ready_sem,
):
    me = lax.axis_index("seq")
    odd = lax.axis_index("head") % 2 == 1
    rows, width = q_ref.shape
    tokens = rows // heads
    half = tokens // 2
    per_group = heads // groups
    cols = tokens * groups
    per_side = recv_sem.shape[1] // 2
    piece = cols // per_side
    factor_scale = width ** (-0.5) * math.log2(math.e)
    has_right, has_left = me < n - 1, me > 0
    reach_left, reach_right = min(3, n - 1), min(2, n - 1)
    barrier = pltpu.get_barrier_semaphore()

    loads = [
        pltpu.make_async_copy(k_hbm, kv_ref.at[me, KEYS], load_sem.at[0]),
        pltpu.make_async_copy(v_hbm, kv_ref.at[me, VALUES], load_sem.at[0]),
        pltpu.make_async_copy(table_hbm, table_ref, load_sem.at[1]),
        pltpu.make_async_copy(q_hbm, q_ref, load_sem.at[2]),
    ]
    for load in loads:
        load.start()

    def straight_left(high, low, is_odd):
        far = high - low
        even_way = far <= reach_left
        odd_way = (far == 1) | ((far == 2) & (high == n - 1))
        return (low >= 0) & (high < n) & ((is_odd & odd_way) | (jnp.logical_not(is_odd) & even_way))

    def straight_right(low, high):
        return (low >= 0) & (high < n) & (high - low <= reach_right)

    def meets(high, low):
        return straight_left(high, low, odd) | straight_right(low, high)

    for k in range(1, reach_left + 1):

        @pl.when(meets(me + k, me))
        def _():
            pl.semaphore_signal(barrier, inc=1, device_id={"seq": me + k}, device_id_type=MESH)

    greeted = [meets(me, me - k).astype(jnp.int32) for k in range(1, reach_left + 1)]

    @pl.when(has_left)
    def _():
        pl.semaphore_wait(barrier, sum(greeted))

    for k in range(1, reach_right + 1):

        @pl.when(straight_right(me - k, me))
        def _():
            pl.semaphore_signal(
                ready_sem.at[k - 1], inc=1, device_id={"seq": me - k}, device_id_type=MESH
            )

    def remote(shard, side, index, target, source=None):
        part = kv_ref.at[shard, side, pl.ds(index * piece, piece)]
        slot = jnp.where(shard < target, shard, shard - 1)
        return pltpu.make_async_remote_copy(
            src_ref=part if source is None else source.at[pl.ds(index * piece, piece)],
            dst_ref=part,
            send_sem=send_sem.at[jnp.where(target < me, 0, 1)],
            recv_sem=recv_sem.at[slot, side * per_side + index],
            device_id={"seq": target},
            device_id_type=MESH,
        )

    def send_mine(target, allowed, sources=(None, None)):
        @pl.when(allowed)
        def _():
            for side in (KEYS, VALUES):
                for index in range(per_side):
                    remote(me, side, index, target, sources[side]).start()

    for k, rank in ((3, None), (2, False), (1, None), (2, True)):
        if k <= reach_left:
            turn = straight_left(me, me - k, odd)
            if rank is not None:
                turn &= (jnp.logical_not(odd) & (me == n - 1)) == rank
            send_mine(me - k, turn, (k_hbm, v_hbm))

    m_ref[...] = jnp.full(m_ref.shape, NEG, jnp.float32)
    l_ref[...] = jnp.zeros(l_ref.shape, jnp.float32)
    acc_ref[...] = jnp.zeros(acc_ref.shape, jnp.float32)
    pltpu.make_async_copy(kv_ref.at[me], kv_ref.at[me], load_sem.at[0]).wait()
    loads[2].wait()
    loads[3].wait()

    lane = lax.broadcasted_iota(jnp.int32, (heads, tokens), 1)
    group = lax.broadcasted_iota(jnp.int32, (heads, tokens), 0) // per_group
    spans = [(pl.ds(start * heads, tile * heads), start) for start in range(0, tokens, tile)]

    def by_group(shard, side):
        wide_ref[...] = kv_ref[shard, side].astype(jnp.float32)
        split = [wide_ref[pl.ds(g, tokens, stride=groups), :] for g in range(groups)]
        return jnp.concatenate(split, axis=0).astype(kv_ref.dtype)

    def scores(shard, span, start, mine=False, closes=False):
        section = start // half
        first, second = table_ref[2 * shard], table_ref[2 * shard + 1]
        key_pos = jnp.where(lane < half, first * half + lane, (second - 1) * half + lane)
        offset = table_ref[2 * me + section] * half + start % half
        raw = lax.dot_general(
            q_ref[span, :],
            keys_ref[...],
            (((1,), (1,)), ((), ())),
            preferred_element_type=jnp.float32,
        )
        raw = raw.reshape(tile, heads, cols)
        shaped = raw[:, :, :tokens]
        for g in range(1, groups):
            shaped = jnp.where(group[None] == g, raw[:, :, g * tokens : (g + 1) * tokens], shaped)
        if mine:
            query_pos = lax.broadcasted_iota(jnp.int32, shaped.shape, 0) + offset
            shaped = jnp.where(key_pos[None] <= query_pos, shaped, NEG)
        else:
            shaped += jnp.where(key_pos <= offset, 0.0, NEG)[None]
        raw = shaped.reshape(tile * heads, tokens)
        old_max = m_ref[span, :]
        new_max = jnp.maximum(old_max, jnp.max(raw, axis=-1, keepdims=True))
        fade = jnp.exp2((old_max - new_max) * factor_scale)
        weights = jnp.exp2((raw - new_max) * factor_scale)
        sums = l_ref[span, :] * fade + weights
        if not closes:
            m_ref[span, :] = new_max
            l_ref[span, :] = sums
        shaped = weights.reshape(tile, heads, tokens)
        spread = [jnp.where(group[None] == g, shaped, 0.0) for g in range(groups)]
        spread = jnp.concatenate(spread, axis=-1).reshape(tile * heads, cols)
        return spread.astype(p_ref.dtype), fade, sums

    def scale_of(sums):
        high = sums.astype(p_ref.dtype)
        low = (sums - high.astype(jnp.float32)).astype(p_ref.dtype)
        ones = jnp.ones((2 * tokens, width), p_ref.dtype)
        return 1.0 / jnp.dot(
            jnp.concatenate([high, low], axis=1), ones, preferred_element_type=jnp.float32
        )

    def whole(shard, mine=False):
        keys_ref[...] = by_group(shard, KEYS)
        values_ref[...] = by_group(shard, VALUES)
        for span, start in spans:
            weights, fade, _ = scores(shard, span, start, mine)
            acc_ref[span, :] = acc_ref[span, :] * fade + jnp.dot(
                weights, values_ref[...], preferred_element_type=jnp.float32
            )

    def weigh(shard, place, closes):
        keys_ref[...] = by_group(shard, KEYS)
        for span, start in spans:
            weights, fade, sums = scores(shard, span, start, closes=closes)
            p_ref[place, span, :] = weights
            if closes:
                scale = scale_of(sums)
                fade *= scale
                scale_ref[place, span, :] = scale
                if place == 1:
                    scale_ref[0, span, :] = fade
            acc_ref[span, :] = acc_ref[span, :] * fade

    def product(span, place):
        return jnp.dot(p_ref[place, span, :], values_ref[...], preferred_element_type=jnp.float32)

    def add(shard, place, scales):
        values_ref[...] = by_group(shard, VALUES)
        for span, _ in spans:
            term = product(span, place)
            if scales:
                term *= scale_ref[1, span, :]
            acc_ref[span, :] += term

    whole(me, mine=True)

    far_first = (me == n - 3) & jnp.logical_not(odd)
    for k, rank in ((1, False), (2, None), (1, True)):
        if k <= reach_right:
            turn = straight_right(me, me + k)
            if rank is not None:
                turn &= far_first == rank

            @pl.when(turn)
            def _():
                pl.semaphore_wait(ready_sem.at[k - 1], 1)

            send_mine(me + k, turn)

    def take(shard, side):
        for index in range(per_side):
            remote(shard, side, index, me).wait_recv()

            @pl.when(has_right & (shard < me) & jnp.logical_not(straight_right(shard, me + 1)))
            def _():
                remote(shard, side, index, me + 1).start()

            @pl.when(has_left & (shard > me) & jnp.logical_not(straight_left(shard, me - 1, odd)))
            def _():
                remote(shard, side, index, me - 1).start()

    def settle():
        for d in range(n):
            for is_odd in (False, True):
                lefts = [s for s in range(d + 1, n) if d > 0]
                if is_odd:
                    lefts = [s for s in lefts if not (s == n - 1 and s - d == 1)]
                    own_left = min(d, 2 if d == n - 1 else 1)
                else:
                    lefts = [s for s in lefts if s - d + 1 > reach_left]
                    own_left = min(d, reach_left)
                rights = [s for s in range(d) if d < n - 1 and d + 1 - s > reach_right]
                own_right = min(n - 1 - d, reach_right)
                counts = (own_left + len(lefts), own_right + len(rights))

                @pl.when((me == d) & (odd == is_odd))
                def _():
                    for way, count in enumerate(counts):
                        if count:
                            sent = kv_ref.at[pl.ds(0, count)]
                            pltpu.make_async_copy(sent, sent, send_sem.at[way]).wait()

    if n == 1:
        for span, _ in spans:
            out_ref[span, :] = (acc_ref[span, :] * scale_of(l_ref[span, :])).astype(out_ref.dtype)
        return

    def attend_in_turn(second, last, wait_for):
        if second is not None:
            wait_for(1)
            weigh(second, 1, False)
            wait_for(2)
            add(second, 1, False)
        wait_for(3)
        weigh(last, 0, True)

    if n == len(LINE_OF_FOUR):
        variants = [
            ((me == d) & (odd == (parity == 1)), LINE_OF_FOUR[d][parity])
            for d in range(n)
            for parity in range(2)
        ]
        first, second, last, split = (
            sum(jnp.where(mine, plan[field], 0) for mine, plan in variants) for field in range(4)
        )

        def wait_for(stage, kinds=(0, 1)):
            for mine, plan in variants:
                if plan[3] in kinds and plan[4][stage]:

                    @pl.when(mine)
                    def _():
                        for shard, side in plan[4][stage]:
                            take(shard, side)

        wait_for(0)
        whole(first)

        @pl.when(split == 0)
        def _():
            attend_in_turn(second, last, functools.partial(wait_for, kinds=(0,)))

        @pl.when(split == 1)
        def _():
            wait_for(1, (1,))
            weigh(last, 0, False)
            wait_for(2, (1,))
            weigh(second, 1, True)
            wait_for(3, (1,))
            add(second, 1, True)

        wait_for(4)
    else:
        short = jnp.minimum(me, n - 1 - me)

        def order(index):
            paired = jnp.where(index % 2 == 1, me + (index + 1) // 2, me - index // 2)
            alone = jnp.where(me < n - 1 - me, me + index - short, me - index + short)
            return jnp.where(index <= 2 * short, paired, alone)

        def take_both(index):
            take(order(index), KEYS)
            take(order(index), VALUES)

        def round_of(index, carry):
            take_both(index + 1)
            whole(order(index))
            return carry

        if n > 3:
            take_both(1)
            lax.fori_loop(1, n - 3, round_of, 0)
            whole(order(n - 3))
        last = order(n - 1)

        def wait_for(stage):
            take(order(n - 2) if stage < 3 else last, (stage + 1) % 2)

        attend_in_turn(order(n - 2) if n > 2 else None, last, wait_for)
        wait_for(4)

    values_ref[...] = by_group(last, VALUES)
    for span, _ in spans:
        out_ref[span, :] = (acc_ref[span, :] + product(span, 0) * scale_ref[0, span, :]).astype(
            out_ref.dtype
        )
    settle()


def on_device(queries, keys, values, block_order):
    n = lax.axis_size("seq")
    tokens, heads, width = queries.shape
    groups = keys.shape[1]
    rows, cols = tokens * heads, tokens * groups
    tile = min(64, tokens // 2)
    pieces = 4
    anywhere = pl.BlockSpec(memory_space=pltpu.HBM)
    out = pl.pallas_call(
        functools.partial(gather_attend, n, heads, groups, tile),
        out_shape=pltpu.VMEM((rows, width), queries.dtype),
        in_specs=[anywhere] * 4,
        out_specs=pl.BlockSpec(memory_space=pltpu.VMEM),
        scratch_shapes=[
            pltpu.SMEM(block_order.shape, block_order.dtype),
            pltpu.VMEM((rows, width), queries.dtype),
            pltpu.VMEM((n, 2, cols, width), keys.dtype),
            pltpu.VMEM((2, rows, cols), values.dtype),
            pltpu.VMEM((rows, width), jnp.float32),
            pltpu.VMEM((rows, width), jnp.float32),
            pltpu.VMEM((rows, width), jnp.float32),
            pltpu.VMEM((2, rows, width), jnp.float32),
            pltpu.VMEM((cols, width), jnp.float32),
            pltpu.VMEM((cols, width), keys.dtype),
            pltpu.VMEM((cols, width), values.dtype),
            pltpu.SemaphoreType.DMA((3,)),
            pltpu.SemaphoreType.DMA((2,)),
            pltpu.SemaphoreType.DMA((max(n - 1, 1), pieces)),
            pltpu.SemaphoreType.REGULAR((2,)),
        ],
        compiler_params=pltpu.CompilerParams(collective_id=0, has_side_effects=True),
    )(
        block_order,
        queries.reshape(rows, width),
        keys.reshape(cols, width),
        values.reshape(cols, width),
    )
    return out.reshape(tokens, heads, width)


def solution(mesh):
    placed = P(("grp", "seq"), "head", None)
    return jax.shard_map(
        on_device,
        mesh=mesh,
        in_specs=(placed, placed, placed, P("grp")),
        out_specs=placed,
        check_vma=False,
    )
```

```python
import functools
import math

import jax
import jax.numpy as jnp
from jax import lax
from jax.experimental import pallas as pl
from jax.experimental.pallas import tpu as pltpu
from jax.sharding import PartitionSpec as P

MESH = pl.DeviceIdType.MESH
NEG = -1e30
KEYS, VALUES = 0, 1

LINE_OF_FOUR = (
    (
        (1, 3, 2, 0, (((1, KEYS), (1, VALUES)), ((3, KEYS),), ((3, VALUES),), ((2, KEYS),), ((2, VALUES),))),
        (1, 3, 2, 1, (((1, KEYS), (1, VALUES)), ((2, KEYS),), ((3, KEYS),), ((3, VALUES),), ((2, VALUES),))),
    ),
    (
        (0, 3, 2, 1, (((0, KEYS), (0, VALUES)), ((2, KEYS),), ((3, KEYS),), ((3, VALUES),), ((2, VALUES),))),
        (3, 2, 0, 0, (((2, KEYS), (3, KEYS), (3, VALUES), (2, VALUES)), (), (), ((0, KEYS),), ((0, VALUES),))),
    ),
    (
        (0, 3, 1, 0, (((0, KEYS), (0, VALUES)), ((3, KEYS),), ((3, VALUES),), ((1, KEYS),), ((1, VALUES),))),
        (0, 3, 1, 0, (((0, KEYS), (0, VALUES)), ((3, KEYS),), ((3, VALUES),), ((1, KEYS),), ((1, VALUES),))),
    ),
    (
        (2, 1, 0, 0, (((2, KEYS), (2, VALUES)), ((1, KEYS),), ((1, VALUES),), ((0, KEYS),), ((0, VALUES),))),
        (2, 1, 0, 0, (((2, KEYS), (2, VALUES)), ((1, KEYS),), ((1, VALUES),), ((0, KEYS),), ((0, VALUES),))),
    ),
)


def gather_attend(
    n,
    heads,
    groups,
    tile,
    table_hbm,
    q_hbm,
    k_hbm,
    v_hbm,
    out_ref,
    table_ref,
    q_ref,
    kv_ref,
    p_ref,
    m_ref,
    l_ref,
    acc_ref,
    scale_ref,
    wide_ref,
    keys_ref,
    values_ref,
    load_sem,
    send_sem,
    recv_sem,
    ready_sem,
):
    me = lax.axis_index("seq")
    odd = lax.axis_index("head") % 2 == 1
    rows, width = q_ref.shape
    tokens = rows // heads
    half = tokens // 2
    per_group = heads // groups
    cols = tokens * groups
    per_side = recv_sem.shape[1] // 2
    piece = cols // per_side
    factor_scale = width ** (-0.5) * math.log2(math.e)
    has_right, has_left = me < n - 1, me > 0
    reach_left, reach_right = min(3, n - 1), min(2, n - 1)
    barrier = pltpu.get_barrier_semaphore()

    loads = [
        pltpu.make_async_copy(k_hbm, kv_ref.at[me, KEYS], load_sem.at[0]),
        pltpu.make_async_copy(v_hbm, kv_ref.at[me, VALUES], load_sem.at[0]),
        pltpu.make_async_copy(table_hbm, table_ref, load_sem.at[1]),
        pltpu.make_async_copy(q_hbm, q_ref, load_sem.at[0]),
    ]
    for load in loads:
        load.start()

    def straight_left(high, low, is_odd):
        far = high - low
        even_way = far <= reach_left
        odd_way = (far == 1) | ((far == 2) & (high == n - 1))
        return (low >= 0) & (high < n) & ((is_odd & odd_way) | (jnp.logical_not(is_odd) & even_way))

    def straight_right(low, high):
        return (low >= 0) & (high < n) & (high - low <= reach_right)

    def meets(high, low):
        return straight_left(high, low, odd) | straight_right(low, high)

    for k in range(1, reach_left + 1):

        @pl.when(meets(me + k, me))
        def _():
            pl.semaphore_signal(barrier, inc=1, device_id={"seq": me + k}, device_id_type=MESH)

    greeted = [meets(me, me - k).astype(jnp.int32) for k in range(1, reach_left + 1)]

    @pl.when(has_left)
    def _():
        pl.semaphore_wait(barrier, sum(greeted))

    for k in range(1, reach_right + 1):

        @pl.when(straight_right(me - k, me))
        def _():
            pl.semaphore_signal(
                ready_sem.at[k - 1], inc=1, device_id={"seq": me - k}, device_id_type=MESH
            )

    def remote(shard, side, index, target, source=None):
        part = kv_ref.at[shard, side, pl.ds(index * piece, piece)]
        slot = jnp.where(shard < target, shard, shard - 1)
        return pltpu.make_async_remote_copy(
            src_ref=part if source is None else source.at[pl.ds(index * piece, piece)],
            dst_ref=part,
            send_sem=send_sem.at[0 if send_sem.shape[0] == 1 else jnp.where(target < me, 0, 1)],
            recv_sem=recv_sem.at[slot, side * per_side + index],
            device_id={"seq": target},
            device_id_type=MESH,
        )

    def send_mine(target, allowed, sources=(None, None)):
        @pl.when(allowed)
        def _():
            for side in (KEYS, VALUES):
                for index in range(per_side):
                    remote(me, side, index, target, sources[side]).start()

    for k, rank in ((3, None), (2, False), (1, None), (2, True)):
        if k <= reach_left:
            turn = straight_left(me, me - k, odd)
            if rank is not None:
                turn &= (jnp.logical_not(odd) & (me == n - 1)) == rank
            send_mine(me - k, turn, (k_hbm, v_hbm))

    m_ref[...] = jnp.full(m_ref.shape, NEG, jnp.float32)
    l_ref[...] = jnp.zeros(l_ref.shape, jnp.float32)
    acc_ref[...] = jnp.zeros(acc_ref.shape, jnp.float32)
    loaded = p_ref.at[0, pl.ds(0, (2 * cols + rows) * width // cols)]
    pltpu.make_async_copy(loaded, loaded, load_sem.at[0]).wait()
    loads[2].wait()

    lane = lax.broadcasted_iota(jnp.int32, (heads, tokens), 1)
    group = lax.broadcasted_iota(jnp.int32, (heads, tokens), 0) // per_group
    spans = [(pl.ds(start * heads, tile * heads), start) for start in range(0, tokens, tile)]

    def by_group(shard, side):
        wide_ref[...] = kv_ref[shard, side].astype(jnp.float32)
        split = [wide_ref[pl.ds(g, tokens, stride=groups), :] for g in range(groups)]
        return jnp.concatenate(split, axis=0).astype(kv_ref.dtype)

    def scores(shard, span, start, mine=False, closes=False):
        section = start // half
        first, second = table_ref[2 * shard], table_ref[2 * shard + 1]
        key_pos = jnp.where(lane < half, first * half + lane, (second - 1) * half + lane)
        offset = table_ref[2 * me + section] * half + start % half
        raw = lax.dot_general(
            q_ref[span, :],
            keys_ref[...],
            (((1,), (1,)), ((), ())),
            preferred_element_type=jnp.float32,
        )
        raw = raw.reshape(tile, heads, cols)
        shaped = raw[:, :, :tokens]
        for g in range(1, groups):
            shaped = jnp.where(group[None] == g, raw[:, :, g * tokens : (g + 1) * tokens], shaped)
        if mine:
            query_pos = lax.broadcasted_iota(jnp.int32, shaped.shape, 0) + offset
            shaped = jnp.where(key_pos[None] <= query_pos, shaped, NEG)
        else:
            shaped += jnp.where(key_pos <= offset, 0.0, NEG)[None]
        raw = shaped.reshape(tile * heads, tokens)
        old_max = m_ref[span, :]
        new_max = jnp.maximum(old_max, jnp.max(raw, axis=-1, keepdims=True))
        fade = jnp.exp2((old_max - new_max) * factor_scale)
        weights = jnp.exp2((raw - new_max) * factor_scale)
        sums = l_ref[span, :] * fade + weights
        if not closes:
            m_ref[span, :] = new_max
            l_ref[span, :] = sums
        shaped = weights.reshape(tile, heads, tokens)
        spread = [jnp.where(group[None] == g, shaped, 0.0) for g in range(groups)]
        spread = jnp.concatenate(spread, axis=-1).reshape(tile * heads, cols)
        return spread.astype(p_ref.dtype), fade, sums

    def scale_of(sums):
        high = sums.astype(p_ref.dtype)
        low = (sums - high.astype(jnp.float32)).astype(p_ref.dtype)
        ones = jnp.ones((2 * tokens, width), p_ref.dtype)
        return 1.0 / jnp.dot(
            jnp.concatenate([high, low], axis=1), ones, preferred_element_type=jnp.float32
        )

    def whole(shard, mine=False):
        keys_ref[...] = by_group(shard, KEYS)
        values_ref[...] = by_group(shard, VALUES)
        for span, start in spans:
            weights, fade, _ = scores(shard, span, start, mine)
            acc_ref[span, :] = acc_ref[span, :] * fade + jnp.dot(
                weights, values_ref[...], preferred_element_type=jnp.float32
            )

    def weigh(shard, place, closes):
        keys_ref[...] = by_group(shard, KEYS)
        for span, start in spans:
            weights, fade, sums = scores(shard, span, start, closes=closes)
            p_ref[place, span, :] = weights
            if closes:
                scale = scale_of(sums)
                fade *= scale
                scale_ref[place, span, :] = scale
                if place == 1:
                    scale_ref[0, span, :] = fade
            acc_ref[span, :] = acc_ref[span, :] * fade

    def product(span, place):
        return jnp.dot(p_ref[place, span, :], values_ref[...], preferred_element_type=jnp.float32)

    def add(shard, place, scales):
        values_ref[...] = by_group(shard, VALUES)
        for span, _ in spans:
            term = product(span, place)
            if scales:
                term *= scale_ref[1, span, :]
            acc_ref[span, :] += term

    whole(me, mine=True)

    far_first = (me == n - 3) & jnp.logical_not(odd)
    for k, rank in ((1, False), (2, None), (1, True)):
        if k <= reach_right:
            turn = straight_right(me, me + k)
            if rank is not None:
                turn &= far_first == rank

            @pl.when(turn)
            def _():
                pl.semaphore_wait(ready_sem.at[k - 1], 1)

            send_mine(me + k, turn)

    def take(shard, side):
        for index in range(per_side):
            remote(shard, side, index, me).wait_recv()

            @pl.when(has_right & (shard < me) & jnp.logical_not(straight_right(shard, me + 1)))
            def _():
                remote(shard, side, index, me + 1).start()

            @pl.when(has_left & (shard > me) & jnp.logical_not(straight_left(shard, me - 1, odd)))
            def _():
                remote(shard, side, index, me - 1).start()

    def settle():
        for d in range(n):
            for is_odd in (False, True):
                lefts = [s for s in range(d + 1, n) if d > 0]
                if is_odd:
                    lefts = [s for s in lefts if not (s == n - 1 and s - d == 1)]
                    own_left = min(d, 2 if d == n - 1 else 1)
                else:
                    lefts = [s for s in lefts if s - d + 1 > reach_left]
                    own_left = min(d, reach_left)
                rights = [s for s in range(d) if d < n - 1 and d + 1 - s > reach_right]
                own_right = min(n - 1 - d, reach_right)
                counts = (own_left + len(lefts), own_right + len(rights))

                @pl.when((me == d) & (odd == is_odd))
                def _():
                    if send_sem.shape[0] == 1:
                        counts_of = (scale_ref.at[:, pl.ds(0, sum(counts) * cols // 2)],)
                    else:
                        counts_of = [kv_ref.at[pl.ds(0, c)] if c else None for c in counts]
                    for way, sent in enumerate(counts_of):
                        if sent is not None:
                            pltpu.make_async_copy(sent, sent, send_sem.at[way]).wait()

    if n == 1:
        for span, _ in spans:
            out_ref[span, :] = (acc_ref[span, :] * scale_of(l_ref[span, :])).astype(out_ref.dtype)
        return

    def attend_in_turn(second, last, wait_for):
        if second is not None:
            wait_for(1)
            weigh(second, 1, False)
            wait_for(2)
            add(second, 1, False)
        wait_for(3)
        weigh(last, 0, True)

    if n == len(LINE_OF_FOUR):
        variants = [
            ((me == d) & (odd == (parity == 1)), LINE_OF_FOUR[d][parity])
            for d in range(n)
            for parity in range(2)
        ]
        first, second, last, split = (
            sum(jnp.where(mine, plan[field], 0) for mine, plan in variants) for field in range(4)
        )

        def wait_for(stage, kinds=(0, 1)):
            for mine, plan in variants:
                if plan[3] in kinds and plan[4][stage]:

                    @pl.when(mine)
                    def _():
                        for shard, side in plan[4][stage]:
                            take(shard, side)

        wait_for(0)
        whole(first)

        @pl.when(split == 0)
        def _():
            attend_in_turn(second, last, functools.partial(wait_for, kinds=(0,)))

        @pl.when(split == 1)
        def _():
            wait_for(1, (1,))
            weigh(last, 0, False)
            wait_for(2, (1,))
            weigh(second, 1, True)
            wait_for(3, (1,))
            add(second, 1, True)

        wait_for(4)
    else:
        short = jnp.minimum(me, n - 1 - me)

        def order(index):
            paired = jnp.where(index % 2 == 1, me + (index + 1) // 2, me - index // 2)
            alone = jnp.where(me < n - 1 - me, me + index - short, me - index + short)
            return jnp.where(index <= 2 * short, paired, alone)

        def take_both(index):
            take(order(index), KEYS)
            take(order(index), VALUES)

        def round_of(index, carry):
            take_both(index + 1)
            whole(order(index))
            return carry

        if n > 3:
            take_both(1)
            lax.fori_loop(1, n - 3, round_of, 0)
            whole(order(n - 3))
        last = order(n - 1)

        def wait_for(stage):
            take(order(n - 2) if stage < 3 else last, (stage + 1) % 2)

        attend_in_turn(order(n - 2) if n > 2 else None, last, wait_for)
        wait_for(4)

    values_ref[...] = by_group(last, VALUES)
    for span, _ in spans:
        out_ref[span, :] = (acc_ref[span, :] + product(span, 0) * scale_ref[0, span, :]).astype(
            out_ref.dtype
        )
    settle()


def on_device(queries, keys, values, block_order):
    n = lax.axis_size("seq")
    tokens, heads, width = queries.shape
    groups = keys.shape[1]
    rows, cols = tokens * heads, tokens * groups
    tile = min(64, tokens // 2)
    pieces = 4
    anywhere = pl.BlockSpec(memory_space=pltpu.HBM)
    out = pl.pallas_call(
        functools.partial(gather_attend, n, heads, groups, tile),
        out_shape=pltpu.VMEM((rows, width), queries.dtype),
        in_specs=[anywhere] * 4,
        out_specs=pl.BlockSpec(memory_space=pltpu.VMEM),
        scratch_shapes=[
            pltpu.SMEM(block_order.shape, block_order.dtype),
            pltpu.VMEM((rows, width), queries.dtype),
            pltpu.VMEM((n, 2, cols, width), keys.dtype),
            pltpu.VMEM((2, rows, cols), values.dtype),
            pltpu.VMEM((rows, width), jnp.float32),
            pltpu.VMEM((rows, width), jnp.float32),
            pltpu.VMEM((rows, width), jnp.float32),
            pltpu.VMEM((2, rows, width), jnp.float32),
            pltpu.VMEM((cols, width), jnp.float32),
            pltpu.VMEM((cols, width), keys.dtype),
            pltpu.VMEM((cols, width), values.dtype),
            pltpu.SemaphoreType.DMA((2,)),
            pltpu.SemaphoreType.DMA((1 if n <= len(LINE_OF_FOUR) else 2,)),
            pltpu.SemaphoreType.DMA((max(n - 1, 1), pieces)),
            pltpu.SemaphoreType.REGULAR((2,)),
        ],
        compiler_params=pltpu.CompilerParams(collective_id=0, has_side_effects=True),
    )(
        block_order,
        queries.reshape(rows, width),
        keys.reshape(cols, width),
        values.reshape(cols, width),
    )
    return out.reshape(tokens, heads, width)


def solution(mesh):
    placed = P(("grp", "seq"), "head", None)
    return jax.shard_map(
        on_device,
        mesh=mesh,
        in_specs=(placed, placed, placed, P("grp")),
        out_specs=placed,
        check_vma=False,
    )
```

```python
import functools
import math

import jax
import jax.numpy as jnp
from jax import lax
from jax.experimental import pallas as pl
from jax.experimental.pallas import tpu as pltpu
from jax.sharding import PartitionSpec as P

MESH = pl.DeviceIdType.MESH
NEG = -1e30
KEYS, VALUES = 0, 1

LINE_OF_FOUR = (
    (
        (1, 3, 2, 0, (((1, KEYS), (1, VALUES)), ((3, KEYS),), ((3, VALUES),), ((2, KEYS),), ((2, VALUES),))),
        (1, 3, 2, 1, (((1, KEYS), (1, VALUES)), ((2, KEYS),), ((3, KEYS),), ((3, VALUES),), ((2, VALUES),))),
    ),
    (
        (0, 3, 2, 1, (((0, KEYS), (0, VALUES)), ((2, KEYS),), ((3, KEYS),), ((3, VALUES),), ((2, VALUES),))),
        (3, 2, 0, 0, (((2, KEYS), (3, KEYS), (3, VALUES), (2, VALUES)), (), (), ((0, KEYS),), ((0, VALUES),))),
    ),
    (
        (0, 3, 1, 0, (((0, KEYS), (0, VALUES)), ((3, KEYS),), ((3, VALUES),), ((1, KEYS),), ((1, VALUES),))),
        (0, 3, 1, 0, (((0, KEYS), (0, VALUES)), ((3, KEYS),), ((3, VALUES),), ((1, KEYS),), ((1, VALUES),))),
    ),
    (
        (2, 1, 0, 0, (((2, KEYS), (2, VALUES)), ((1, KEYS),), ((1, VALUES),), ((0, KEYS),), ((0, VALUES),))),
        (2, 1, 0, 0, (((2, KEYS), (2, VALUES)), ((1, KEYS),), ((1, VALUES),), ((0, KEYS),), ((0, VALUES),))),
    ),
)


def gather_attend(
    n,
    heads,
    groups,
    tile,
    table_hbm,
    q_hbm,
    k_hbm,
    v_hbm,
    out_ref,
    table_ref,
    q_ref,
    kv_ref,
    p_ref,
    m_ref,
    l_ref,
    acc_ref,
    scale_ref,
    wide_ref,
    keys_ref,
    values_ref,
    load_sem,
    send_sem,
    recv_sem,
    ready_sem,
):
    me = lax.axis_index("seq")
    odd = lax.axis_index("head") % 2 == 1
    rows, width = q_ref.shape
    tokens = rows // heads
    half = tokens // 2
    per_group = heads // groups
    cols = tokens * groups
    per_side = recv_sem.shape[1] // 2
    piece = cols // per_side
    factor_scale = width ** (-0.5) * math.log2(math.e)
    has_right, has_left = me < n - 1, me > 0
    reach_left, reach_right = min(3, n - 1), min(2, n - 1)
    barrier = pltpu.get_barrier_semaphore()

    def straight_left(high, low, is_odd):
        far = high - low
        even_way = far <= reach_left
        odd_way = (far == 1) | ((far == 2) & (high == n - 1))
        return (low >= 0) & (high < n) & ((is_odd & odd_way) | (jnp.logical_not(is_odd) & even_way))

    def straight_right(low, high):
        return (low >= 0) & (high < n) & (high - low <= reach_right)

    def meets(high, low):
        return straight_left(high, low, odd) | straight_right(low, high)

    for k in range(1, reach_left + 1):

        @pl.when(meets(me + k, me))
        def _():
            pl.semaphore_signal(barrier, inc=1, device_id={"seq": me + k}, device_id_type=MESH)

    greeted = [meets(me, me - k).astype(jnp.int32) for k in range(1, reach_left + 1)]

    @pl.when(has_left)
    def _():
        pl.semaphore_wait(barrier, sum(greeted))

    def remote(shard, side, index, target, source=None):
        part = kv_ref.at[shard, side, pl.ds(index * piece, piece)]
        slot = jnp.where(shard < target, shard, shard - 1)
        return pltpu.make_async_remote_copy(
            src_ref=part if source is None else source.at[pl.ds(index * piece, piece)],
            dst_ref=part,
            send_sem=send_sem.at[0 if send_sem.shape[0] == 1 else jnp.where(target < me, 0, 1)],
            recv_sem=recv_sem.at[slot, side * per_side + index],
            device_id={"seq": target},
            device_id_type=MESH,
        )

    def send_mine(target, allowed, sources=(None, None)):
        @pl.when(allowed)
        def _():
            for side in (KEYS, VALUES):
                for index in range(per_side):
                    remote(me, side, index, target, sources[side]).start()

    for k, rank in ((3, None), (2, False), (1, None), (2, True)):
        if k <= reach_left:
            turn = straight_left(me, me - k, odd)
            if rank is not None:
                turn &= (jnp.logical_not(odd) & (me == n - 1)) == rank
            send_mine(me - k, turn, (k_hbm, v_hbm))

    for k in range(1, reach_right + 1):

        @pl.when(straight_right(me - k, me))
        def _():
            pl.semaphore_signal(
                ready_sem.at[k - 1], inc=1, device_id={"seq": me - k}, device_id_type=MESH
            )

    loads = [
        pltpu.make_async_copy(k_hbm, kv_ref.at[me, KEYS], load_sem.at[0]),
        pltpu.make_async_copy(v_hbm, kv_ref.at[me, VALUES], load_sem.at[0]),
        pltpu.make_async_copy(table_hbm, table_ref, load_sem.at[1]),
        pltpu.make_async_copy(q_hbm, q_ref, load_sem.at[0]),
    ]
    for load in loads:
        load.start()

    m_ref[...] = jnp.full(m_ref.shape, NEG, jnp.float32)
    l_ref[...] = jnp.zeros(l_ref.shape, jnp.float32)
    acc_ref[...] = jnp.zeros(acc_ref.shape, jnp.float32)
    loaded = p_ref.at[0, pl.ds(0, (2 * cols + rows) * width // cols)]
    pltpu.make_async_copy(loaded, loaded, load_sem.at[0]).wait()
    loads[2].wait()

    lane = lax.broadcasted_iota(jnp.int32, (heads, tokens), 1)
    group = lax.broadcasted_iota(jnp.int32, (heads, tokens), 0) // per_group
    spans = [(pl.ds(start * heads, tile * heads), start) for start in range(0, tokens, tile)]

    def by_group(shard, side):
        wide_ref[...] = kv_ref[shard, side].astype(jnp.float32)
        split = [wide_ref[pl.ds(g, tokens, stride=groups), :] for g in range(groups)]
        return jnp.concatenate(split, axis=0).astype(kv_ref.dtype)

    def scores(shard, span, start, mine=False, closes=False):
        section = start // half
        first, second = table_ref[2 * shard], table_ref[2 * shard + 1]
        key_pos = jnp.where(lane < half, first * half + lane, (second - 1) * half + lane)
        offset = table_ref[2 * me + section] * half + start % half
        raw = lax.dot_general(
            q_ref[span, :],
            keys_ref[...],
            (((1,), (1,)), ((), ())),
            preferred_element_type=jnp.float32,
        )
        raw = raw.reshape(tile, heads, cols)
        shaped = raw[:, :, :tokens]
        for g in range(1, groups):
            shaped = jnp.where(group[None] == g, raw[:, :, g * tokens : (g + 1) * tokens], shaped)
        if mine:
            query_pos = lax.broadcasted_iota(jnp.int32, shaped.shape, 0) + offset
            shaped = jnp.where(key_pos[None] <= query_pos, shaped, NEG)
        else:
            shaped += jnp.where(key_pos <= offset, 0.0, NEG)[None]
        raw = shaped.reshape(tile * heads, tokens)
        old_max = m_ref[span, :]
        new_max = jnp.maximum(old_max, jnp.max(raw, axis=-1, keepdims=True))
        fade = jnp.exp2((old_max - new_max) * factor_scale)
        weights = jnp.exp2((raw - new_max) * factor_scale)
        sums = l_ref[span, :] * fade + weights
        if not closes:
            m_ref[span, :] = new_max
            l_ref[span, :] = sums
        shaped = weights.reshape(tile, heads, tokens)
        spread = [jnp.where(group[None] == g, shaped, 0.0) for g in range(groups)]
        spread = jnp.concatenate(spread, axis=-1).reshape(tile * heads, cols)
        return spread.astype(p_ref.dtype), fade, sums

    def scale_of(sums):
        high = sums.astype(p_ref.dtype)
        low = (sums - high.astype(jnp.float32)).astype(p_ref.dtype)
        ones = jnp.ones((2 * tokens, width), p_ref.dtype)
        return 1.0 / jnp.dot(
            jnp.concatenate([high, low], axis=1), ones, preferred_element_type=jnp.float32
        )

    def whole(shard, mine=False):
        keys_ref[...] = by_group(shard, KEYS)
        values_ref[...] = by_group(shard, VALUES)
        for span, start in spans:
            weights, fade, _ = scores(shard, span, start, mine)
            acc_ref[span, :] = acc_ref[span, :] * fade + jnp.dot(
                weights, values_ref[...], preferred_element_type=jnp.float32
            )

    def weigh(shard, place, closes):
        keys_ref[...] = by_group(shard, KEYS)
        for span, start in spans:
            weights, fade, sums = scores(shard, span, start, closes=closes)
            p_ref[place, span, :] = weights
            if closes:
                scale = scale_of(sums)
                fade *= scale
                scale_ref[place, span, :] = scale
                if place == 1:
                    scale_ref[0, span, :] = fade
            acc_ref[span, :] = acc_ref[span, :] * fade

    def product(span, place):
        return jnp.dot(p_ref[place, span, :], values_ref[...], preferred_element_type=jnp.float32)

    def add(shard, place, scales):
        values_ref[...] = by_group(shard, VALUES)
        for span, _ in spans:
            term = product(span, place)
            if scales:
                term *= scale_ref[1, span, :]
            acc_ref[span, :] += term

    whole(me, mine=True)

    far_first = (me == n - 3) & jnp.logical_not(odd)
    for k, rank in ((1, False), (2, None), (1, True)):
        if k <= reach_right:
            turn = straight_right(me, me + k)
            if rank is not None:
                turn &= far_first == rank

            @pl.when(turn)
            def _():
                pl.semaphore_wait(ready_sem.at[k - 1], 1)

            send_mine(me + k, turn)

    def take(shard, side):
        for index in range(per_side):
            remote(shard, side, index, me).wait_recv()

            @pl.when(has_right & (shard < me) & jnp.logical_not(straight_right(shard, me + 1)))
            def _():
                remote(shard, side, index, me + 1).start()

            @pl.when(has_left & (shard > me) & jnp.logical_not(straight_left(shard, me - 1, odd)))
            def _():
                remote(shard, side, index, me - 1).start()

    def settle():
        for d in range(n):
            for is_odd in (False, True):
                lefts = [s for s in range(d + 1, n) if d > 0]
                if is_odd:
                    lefts = [s for s in lefts if not (s == n - 1 and s - d == 1)]
                    own_left = min(d, 2 if d == n - 1 else 1)
                else:
                    lefts = [s for s in lefts if s - d + 1 > reach_left]
                    own_left = min(d, reach_left)
                rights = [s for s in range(d) if d < n - 1 and d + 1 - s > reach_right]
                own_right = min(n - 1 - d, reach_right)
                counts = (own_left + len(lefts), own_right + len(rights))

                @pl.when((me == d) & (odd == is_odd))
                def _():
                    if send_sem.shape[0] == 1:
                        counts_of = (scale_ref.at[:, pl.ds(0, sum(counts) * cols // 2)],)
                    else:
                        counts_of = [kv_ref.at[pl.ds(0, c)] if c else None for c in counts]
                    for way, sent in enumerate(counts_of):
                        if sent is not None:
                            pltpu.make_async_copy(sent, sent, send_sem.at[way]).wait()

    if n == 1:
        for span, _ in spans:
            out_ref[span, :] = (acc_ref[span, :] * scale_of(l_ref[span, :])).astype(out_ref.dtype)
        return

    def attend_in_turn(second, last, wait_for):
        if second is not None:
            wait_for(1)
            weigh(second, 1, False)
            wait_for(2)
            add(second, 1, False)
        wait_for(3)
        weigh(last, 0, True)

    if n == len(LINE_OF_FOUR):
        variants = [
            ((me == d) & (odd == (parity == 1)), LINE_OF_FOUR[d][parity])
            for d in range(n)
            for parity in range(2)
        ]
        first, second, last, split = (
            sum(jnp.where(mine, plan[field], 0) for mine, plan in variants) for field in range(4)
        )

        def wait_for(stage, kinds=(0, 1)):
            for mine, plan in variants:
                if plan[3] in kinds and plan[4][stage]:

                    @pl.when(mine)
                    def _():
                        for shard, side in plan[4][stage]:
                            take(shard, side)

        wait_for(0)
        whole(first)

        @pl.when(split == 0)
        def _():
            attend_in_turn(second, last, functools.partial(wait_for, kinds=(0,)))

        @pl.when(split == 1)
        def _():
            wait_for(1, (1,))
            weigh(last, 0, False)
            wait_for(2, (1,))
            weigh(second, 1, True)
            wait_for(3, (1,))
            add(second, 1, True)

        wait_for(4)
    else:
        short = jnp.minimum(me, n - 1 - me)

        def order(index):
            paired = jnp.where(index % 2 == 1, me + (index + 1) // 2, me - index // 2)
            alone = jnp.where(me < n - 1 - me, me + index - short, me - index + short)
            return jnp.where(index <= 2 * short, paired, alone)

        def take_both(index):
            take(order(index), KEYS)
            take(order(index), VALUES)

        def round_of(index, carry):
            take_both(index + 1)
            whole(order(index))
            return carry

        if n > 3:
            take_both(1)
            lax.fori_loop(1, n - 3, round_of, 0)
            whole(order(n - 3))
        last = order(n - 1)

        def wait_for(stage):
            take(order(n - 2) if stage < 3 else last, (stage + 1) % 2)

        attend_in_turn(order(n - 2) if n > 2 else None, last, wait_for)
        wait_for(4)

    values_ref[...] = by_group(last, VALUES)
    for span, _ in spans:
        out_ref[span, :] = (acc_ref[span, :] + product(span, 0) * scale_ref[0, span, :]).astype(
            out_ref.dtype
        )
    settle()


def on_device(queries, keys, values, block_order):
    n = lax.axis_size("seq")
    tokens, heads, width = queries.shape
    groups = keys.shape[1]
    rows, cols = tokens * heads, tokens * groups
    tile = min(64, tokens // 2)
    pieces = 4
    anywhere = pl.BlockSpec(memory_space=pltpu.HBM)
    out = pl.pallas_call(
        functools.partial(gather_attend, n, heads, groups, tile),
        out_shape=pltpu.VMEM((rows, width), queries.dtype),
        in_specs=[anywhere] * 4,
        out_specs=pl.BlockSpec(memory_space=pltpu.VMEM),
        scratch_shapes=[
            pltpu.SMEM(block_order.shape, block_order.dtype),
            pltpu.VMEM((rows, width), queries.dtype),
            pltpu.VMEM((n, 2, cols, width), keys.dtype),
            pltpu.VMEM((2, rows, cols), values.dtype),
            pltpu.VMEM((rows, width), jnp.float32),
            pltpu.VMEM((rows, width), jnp.float32),
            pltpu.VMEM((rows, width), jnp.float32),
            pltpu.VMEM((2, rows, width), jnp.float32),
            pltpu.VMEM((cols, width), jnp.float32),
            pltpu.VMEM((cols, width), keys.dtype),
            pltpu.VMEM((cols, width), values.dtype),
            pltpu.SemaphoreType.DMA((2,)),
            pltpu.SemaphoreType.DMA((1 if n <= len(LINE_OF_FOUR) else 2,)),
            pltpu.SemaphoreType.DMA((max(n - 1, 1), pieces)),
            pltpu.SemaphoreType.REGULAR((2,)),
        ],
        compiler_params=pltpu.CompilerParams(collective_id=0, has_side_effects=True),
    )(
        block_order,
        queries.reshape(rows, width),
        keys.reshape(cols, width),
        values.reshape(cols, width),
    )
    return out.reshape(tokens, heads, width)


def solution(mesh):
    placed = P(("grp", "seq"), "head", None)
    return jax.shard_map(
        on_device,
        mesh=mesh,
        in_specs=(placed, placed, placed, P("grp")),
        out_specs=placed,
        check_vma=False,
    )
```
